1024 devices in a mesh: mem: 16 (over x_lo, y), band: 64 (over x_hi, z, core).
Axes of the slice: x: 8 (x_hi: 4, x_lo: 2; x = x_hi * 2 + x_lo), y: 8, z: 8, core: 2. Of those that a mesh axis runs over, the one named last changes fastest.
Arguments:
- ensemble: float32 [64, 4, 256, 1440], P('mem', None, 'band'), may hold values from -6 to 6
- gradient: float32 [4, 1024, 5760], P(None, 'band', 'mem'), may hold values from -60 to 60
- previous: float32 [4, 1024, 5760], P(None, 'band', 'mem'), may hold values from -6 to 6
- diffusivity: float32 [4, 1024, 5760], P(None, 'band', 'mem'), may hold values from 0.03 to 0.12
Outputs:
- analysis: float32 [4, 1024, 5760], P(None, 'band', 'mem')
- direction: float32 [4, 1024, 5760], P(None, 'band', 'mem')
The draws below stay inside these ranges and needn't reach their ends.
All inputs are finite; a program needn't handle non-finite values.
Results may differ from the reference program's by a relative error of at most 0.00012.
Values sent between devices are 32-bit elements; how exact they have to be, the bound alone decides.
No kernel may reach another device: no remote copies, remote signals or barrier semaphores. Data moves between devices by JAX's collectives and lax.ppermute only.
A program may use at most 64 MiB of HBM per device.

```python
import math
import jax
import jax.numpy as jnp
from jax import lax

V = 4
NLON = 1440
REFINE = 4
SUBSTEPS = 16
LSTEPS = 4
LOCLON = 48
M = 64
NCLAT = 256
NFLAT = 1024
NFLON = 5760


def draw_gradient(key, part):
    rough_key = jax.random.fold_in(key, 11)
    column_key = jax.random.fold_in(key, 12)
    row_place = jnp.arange(NFLAT, dtype=jnp.float32) / max(NFLAT - 1, 1)
    row_scale = 0.3 * 10.0 ** row_place
    column_scale = 10.0 ** (jax.random.uniform(column_key, (NFLON,), jnp.float32) - 0.5)
    scales = row_scale[None, :, None] * column_scale[None, None, :]
    rough_part = jnp.clip(jax.random.normal(rough_key, (V, NFLAT, NFLON), jnp.float32), -5.0, 5.0)
    return scales * rough_part


def block_levels(stream_key, shape, split, smallest, largest):
    level, own = 1.0, jax.random.fold_in(stream_key, 6)
    for axis_at, blocks in split:
        steps = jnp.exp(jax.random.uniform(jax.random.fold_in(own, axis_at), (blocks,), jnp.float32, smallest / len(split), largest / len(split)))
        level = level * jnp.repeat(steps, shape[axis_at] // blocks).reshape([-1 if axis == axis_at else 1 for axis in range(len(shape))])
    return level


def centred(own_key, dims, spread, most, split=(), kind=jnp.bfloat16):
    array = jax.random.normal(own_key, dims, jnp.float32) * spread
    if len(split) > 0:
        array = block_levels(own_key, dims, split, -0.22, 0.18) * array
    return jnp.clip(array, min=-most, max=most).astype(kind)


def setup_inputs(seed: int = 0) -> dict:
    streams_of = jax.random.split(jax.random.key(seed), 5)
    ensemble = centred(streams_of[0], (M, V, NCLAT, NLON), 1.0, 6.0, ((0, 16), (2, 64)), jnp.float32)
    gradient = draw_gradient(jax.random.fold_in(streams_of[4], 71), 0)
    previous = centred(streams_of[2], (V, NFLAT, NFLON), 1.0, 6.0, ((1, 64), (2, 16)), jnp.float32)
    diffusivity = jnp.clip(jnp.exp(math.log(0.12) - 1.3862944 * jax.random.uniform(streams_of[3], (V, NFLAT, NFLON), jnp.float32) ** block_levels(streams_of[3], (V, NFLAT, NFLON), ((1, 64), (2, 16)), -0.2, 0.2)), 0.03, 0.12)
    return dict(ensemble=ensemble, gradient=gradient, previous=previous, diffusivity=diffusivity)


LATITUDE_RATE = 0.25
HYBRID_WEIGHT = 0.5

def longitude_kernel(extent, length):
    places = jnp.arange(extent, dtype=jnp.float32)
    spacing = jnp.abs(places[:, None] - places[None, :])
    spacing = jnp.minimum(spacing, extent - spacing)
    return jnp.exp(-0.5 * (spacing / length) ** 2)

def fine_faces(diffusivity):
    total_rows = diffusivity.shape[1]
    east_face = jnp.sqrt(diffusivity * jnp.roll(diffusivity, -1, axis=2))
    west_face = jnp.sqrt(diffusivity * jnp.roll(diffusivity, 1, axis=2))
    north_face = jnp.sqrt(diffusivity * jnp.roll(diffusivity, -1, axis=1))
    south_face = jnp.sqrt(diffusivity * jnp.roll(diffusivity, 1, axis=1))
    row_place = jnp.arange(total_rows, dtype=jnp.int32)[None, :, None]
    north_face = jnp.where(row_place < total_rows - 1, north_face, jnp.zeros_like(north_face))
    south_face = jnp.where(row_place > 0, south_face, jnp.zeros_like(south_face))
    return (east_face, west_face, north_face, south_face)

def fine_substep(state_field, east_face, west_face, north_face, south_face):
    change = east_face * (jnp.roll(state_field, -1, axis=2) - state_field) + west_face * (jnp.roll(state_field, 1, axis=2) - state_field)
    change = change + north_face * (jnp.roll(state_field, -1, axis=1) - state_field) + south_face * (jnp.roll(state_field, 1, axis=1) - state_field)
    return state_field + change

def reference(ensemble, gradient, previous, diffusivity):
    east_face, west_face, north_face, south_face = fine_faces(diffusivity)
    smoothed = gradient
    for sweep_index in range(SUBSTEPS):
        smoothed = fine_substep(smoothed, east_face, west_face, north_face, south_face)
    restricted = gradient.reshape(V, NCLAT, REFINE, NLON, REFINE).sum(axis=(2, 4)) * (1.0 / (REFINE * REFINE))
    control = lax.optimization_barrier(jnp.sum(ensemble * restricted[None], axis=1))
    kernel = longitude_kernel(NLON, LOCLON)
    members = ensemble.shape[0]
    blended = jnp.dot(control.reshape(members * NCLAT, NLON), kernel, precision=lax.Precision.HIGHEST).reshape(members, NCLAT, NLON)
    row_place = jnp.arange(NCLAT, dtype=jnp.int32)[None, :, None]
    north_rate = jnp.where(row_place < NCLAT - 1, LATITUDE_RATE, 0.0).astype(jnp.float32)
    south_rate = jnp.where(row_place > 0, LATITUDE_RATE, 0.0).astype(jnp.float32)
    for sweep_index in range(LSTEPS):
        blended = blended + north_rate * (jnp.roll(blended, -1, axis=1) - blended) + south_rate * (jnp.roll(blended, 1, axis=1) - blended)
    inverse_count = 1.0 / (members - 1)
    ensemble_part = lax.optimization_barrier(jnp.sum(ensemble * blended[:, None], axis=0)) * inverse_count
    injected = jnp.broadcast_to(ensemble_part[:, :, None, :, None], (V, NCLAT, REFINE, NLON, REFINE)).reshape(V, NFLAT, NFLON)
    direction = HYBRID_WEIGHT * smoothed + HYBRID_WEIGHT * injected
    along_sum = jnp.sum(gradient * direction)
    square_sum = jnp.sum(direction * direction)
    analysis = previous - along_sum / (along_sum + square_sum) * direction
    return (analysis, direction)
```

```python
import jax
import jax.numpy as jnp
from jax import lax
from jax.experimental import pallas as pl
from jax.experimental.pallas import tpu as pltpu
from jax.sharding import Mesh
from jax.sharding import PartitionSpec as P

NLON = 1440
REFINE = 4
SUBSTEPS = 16
LSTEPS = 4
LOCLON = 48
BAND = ("band_0", "band_1", "band_2")
MEM = ("mem_0", "mem_1")
ALL = ("mem_0", "mem_1", "band_0", "band_1", "band_2")

LATITUDE_RATE = 0.25
HYBRID_WEIGHT = 0.5
BLOCK = 240
VMEM_LIMIT = 24 << 20


def shifted(block, axis, step):
    count = lax.axis_size(axis)
    return lax.ppermute(block, axis, [(i, (i + step) % count) for i in range(count)])


def everywhere(shard, axis):
    copies = jnp.broadcast_to(shard[None], (lax.axis_size(axis), *shard.shape))
    return lax.all_to_all(copies, axis, split_axis=0, concat_axis=0, tiled=True)


def params():
    return pltpu.CompilerParams(vmem_limit_bytes=VMEM_LIMIT)


def longitude_kernel_body(high_ref, low_ref):
    rows, columns = high_ref.shape
    own = lax.broadcasted_iota(jnp.int32, (rows, columns), 0)
    other = lax.broadcasted_iota(jnp.int32, (rows, columns), 1)
    spacing = jnp.abs(own - other)
    spacing = jnp.minimum(spacing, NLON - spacing).astype(jnp.float32)
    value = jnp.exp(-0.5 * (spacing / LOCLON) ** 2)
    high = value.astype(jnp.bfloat16)
    high_ref[...] = high
    low_ref[...] = (value - high.astype(jnp.float32)).astype(jnp.bfloat16)


def longitude_kernel():
    part = jax.ShapeDtypeStruct((NLON, BLOCK), jnp.bfloat16)
    return pl.pallas_call(
        longitude_kernel_body,
        out_shape=(part, part),
        compiler_params=params(),
        cost_estimate=pl.CostEstimate(
            flops=20 * NLON * BLOCK, transcendentals=NLON * BLOCK, bytes_accessed=4 * NLON * BLOCK
        ),
        name="longitude_kernel",
    )()


def blend_body(ensemble_ref, low_ref, own_ref, high_ref, kernel_high_ref, kernel_low_ref, out_ref, ext_ref):
    members, variables, coarse_rows, columns = ensemble_ref.shape
    ext_rows = coarse_rows + 2 * LSTEPS
    bands = 1
    for axis in BAND:
        bands = bands * lax.axis_size(axis)
    band = lax.axis_index(BAND)
    for m in range(members):
        base = m * ext_rows
        ext_ref[base : base + LSTEPS] = low_ref[m]
        ext_ref[base + LSTEPS : base + LSTEPS + coarse_rows] = own_ref[m]
        ext_ref[base + LSTEPS + coarse_rows : base + ext_rows] = high_ref[m]
    q = ext_ref[...]
    total = members * ext_rows
    place = lax.rem(lax.broadcasted_iota(jnp.int32, (total, 1), 0), ext_rows)
    row = band * coarse_rows - LSTEPS + place
    rows = bands * coarse_rows
    north = jnp.where((row >= 0) & (row < rows - 1), LATITUDE_RATE, 0.0)
    south = jnp.where((row > 0) & (row <= rows - 1), LATITUDE_RATE, 0.0)
    for _ in range(LSTEPS):
        q = (
            q
            + north * (pltpu.roll(q, total - 1, 0) - q)
            + south * (pltpu.roll(q, 1, 0) - q)
        )
    ext_ref[...] = q
    x = jnp.concatenate(
        [
            ext_ref[m * ext_rows + LSTEPS : m * ext_rows + LSTEPS + coarse_rows]
            for m in range(members)
        ],
        axis=0,
    )
    turned = jnp.concatenate(
        [x] + [
            jnp.concatenate([x[:, BLOCK * j :], x[:, : BLOCK * j]], axis=1)
            for j in range(1, NLON // BLOCK)
        ],
        axis=0,
    )
    part = turned.astype(jnp.bfloat16)
    rest = (turned - part.astype(jnp.float32)).astype(jnp.bfloat16)
    kernel_high = kernel_high_ref[...]
    y = jnp.dot(part, kernel_high, preferred_element_type=jnp.float32)
    y = y + jnp.dot(rest, kernel_high, preferred_element_type=jnp.float32)
    y = y + jnp.dot(part, kernel_low_ref[...], preferred_element_type=jnp.float32)
    held = members * coarse_rows
    blended = jnp.concatenate(
        [y[held * j : held * (j + 1)] for j in range(NLON // BLOCK)], axis=1
    )
    for v in range(variables):
        term = ensemble_ref[0, v] * blended[:coarse_rows]
        for m in range(1, members):
            term = term + ensemble_ref[m, v] * blended[m * coarse_rows : (m + 1) * coarse_rows]
        out_ref[v] = term


def blend(ensemble, low, own, high, kernel_high, kernel_low):
    members, variables, coarse_rows, columns = ensemble.shape
    return pl.pallas_call(
        blend_body,
        out_shape=jax.ShapeDtypeStruct((variables, coarse_rows, columns), jnp.float32),
        scratch_shapes=[pltpu.VMEM((members * (coarse_rows + 2 * LSTEPS), columns), jnp.float32)],
        compiler_params=params(),
        cost_estimate=pl.CostEstimate(
            flops=6 * 16 * NLON * NLON, transcendentals=0, bytes_accessed=4 << 20
        ),
        name="blend",
    )(ensemble, low, own, high, kernel_high, kernel_low)


def diffuse_body(low_ref, own_ref, high_ref, out_ref, field_ref, east_ref, north_ref):
    twice, tile_rows, width = own_ref.shape
    variables = twice // 2
    height = 3 * tile_rows
    bands = 1
    for axis in BAND:
        bands = bands * lax.axis_size(axis)
    first = lax.axis_index(BAND) * tile_rows - tile_rows
    row = first + lax.broadcasted_iota(jnp.int32, (height, 1), 0)
    inside = (row >= 0) & (row + 1 <= bands * tile_rows - 1)
    for v in range(variables):
        field_ref[v] = jnp.concatenate([low_ref[v], own_ref[v], high_ref[v]], axis=0)
        w = variables + v
        rate = jnp.concatenate([low_ref[w], own_ref[w], high_ref[w]], axis=0)
        east_ref[v] = jnp.sqrt(rate * pltpu.roll(rate, width - 1, 1))
        north_ref[v] = jnp.where(inside, jnp.sqrt(rate * pltpu.roll(rate, height - 1, 0)), 0.0)

    def substep(_, carry):
        for v in range(variables):
            f = field_ref[v]
            east = east_ref[v] * (pltpu.roll(f, width - 1, 1) - f)
            north = north_ref[v] * (pltpu.roll(f, height - 1, 0) - f)
            change = east - pltpu.roll(east, 1, 1)
            change = change + north - pltpu.roll(north, 1, 0)
            field_ref[v] = f + change
        return carry

    lax.fori_loop(0, SUBSTEPS, substep, 0)
    for v in range(variables):
        out_ref[v] = field_ref[v, tile_rows : 2 * tile_rows, : out_ref.shape[2]]


def diffuse(low, own, high, columns):
    twice, tile_rows, width = own.shape
    variables = twice // 2
    held = pltpu.VMEM((variables, 3 * tile_rows, width), jnp.float32)
    return pl.pallas_call(
        diffuse_body,
        out_shape=jax.ShapeDtypeStruct((variables, tile_rows, columns), jnp.float32),
        scratch_shapes=[held, held, held],
        compiler_params=params(),
        cost_estimate=pl.CostEstimate(
            flops=16 * 12 * variables * 48 * width, transcendentals=0, bytes_accessed=2 << 20
        ),
        name="diffuse",
    )(low, own, high)


def chosen(rows, columns, ratio, by_row):
    own = lax.broadcasted_iota(jnp.int32, (rows, columns), 0)
    other = lax.broadcasted_iota(jnp.int32, (rows, columns), 1)
    same = (other // ratio == own) if by_row else (own // ratio == other)
    return same.astype(jnp.float32)


def shards(ensemble, gradient, previous, diffusivity):
    variables, tile_rows, columns = gradient.shape
    members, _, coarse_rows, _ = ensemble.shape
    coarse_cols = columns // REFINE
    owners = lax.axis_size(MEM)
    row_sums = gradient.reshape(variables * coarse_rows, REFINE, columns).sum(axis=1)
    restricted = jnp.dot(
        row_sums, chosen(columns, coarse_cols, REFINE, False), precision=lax.Precision.HIGHEST
    ) * (1.0 / (REFINE * REFINE))
    gathered = everywhere(restricted.reshape(variables, coarse_rows, coarse_cols), MEM)
    gathered = jnp.moveaxis(gathered, 0, 2).reshape(variables, coarse_rows, NLON)
    both = jnp.concatenate([gradient, diffusivity], axis=0)
    left = shifted(both[:, :, columns - SUBSTEPS :], MEM, 1)
    right = shifted(both[:, :, :SUBSTEPS], MEM, -1)
    spare = -(columns + 2 * SUBSTEPS) % 128
    gap = jnp.zeros((2 * variables, tile_rows, spare), jnp.float32)
    extended = jnp.concatenate([both, right, gap, left], axis=2)
    kernel_high, kernel_low = longitude_kernel()
    control = jnp.sum(ensemble * gathered[None], axis=1)
    control_low = shifted(control, BAND, 1)
    control_high = shifted(control, BAND, -1)
    rows_low = shifted(extended, BAND, 1)
    rows_high = shifted(extended, BAND, -1)
    member_terms = blend(ensemble, control_low, control, control_high, kernel_high, kernel_low)
    blocks = jnp.moveaxis(member_terms.reshape(variables, coarse_rows, owners, coarse_cols), 2, 0)
    arrived = lax.all_to_all(blocks, MEM, split_axis=0, concat_axis=0, tiled=True)
    smoothed = diffuse(rows_low, extended, rows_high, columns)
    inverse_count = 1.0 / (members * owners - 1)
    ensemble_part = arrived.sum(axis=0) * inverse_count
    spread = jnp.dot(
        ensemble_part.reshape(variables * coarse_rows, coarse_cols),
        chosen(coarse_cols, columns, REFINE, True),
        precision=lax.Precision.HIGHEST,
    )
    injected = jnp.broadcast_to(
        spread.reshape(variables, coarse_rows, 1, columns),
        (variables, coarse_rows, REFINE, columns),
    ).reshape(gradient.shape)
    direction = HYBRID_WEIGHT * smoothed + HYBRID_WEIGHT * injected
    along_sum, square_sum = lax.psum(
        (jnp.sum(gradient * direction), jnp.sum(direction * direction)), ALL
    )
    analysis = previous - along_sum / (along_sum + square_sum) * direction
    return (analysis, direction)


def solution(mesh):
    split = Mesh(
        mesh.devices.reshape(2, 8, 4, 8, 2), ("mem_0", "mem_1", "band_0", "band_1", "band_2")
    )
    return jax.shard_map(
        shards,
        mesh=split,
        in_specs=(
            P(MEM, None, BAND, None),
            P(None, BAND, MEM),
            P(None, BAND, MEM),
            P(None, BAND, MEM),
        ),
        out_specs=(P(None, BAND, MEM), P(None, BAND, MEM)),
        check_vma=False,
    )
```

```python
import jax
import jax.numpy as jnp
from jax import lax
from jax.experimental import pallas as pl
from jax.experimental.pallas import tpu as pltpu
from jax.sharding import Mesh
from jax.sharding import PartitionSpec as P

NLON = 1440
REFINE = 4
SUBSTEPS = 16
LSTEPS = 4
LOCLON = 48
BAND = ("band_0", "band_1", "band_2")
MEM = ("mem_0", "mem_1")

LATITUDE_RATE = 0.25
HYBRID_WEIGHT = 0.5
BLOCK = 240
VMEM_LIMIT = 24 << 20


def shifted(block, axis, step):
    count = lax.axis_size(axis)
    return lax.ppermute(block, axis, [(i, (i + step) % count) for i in range(count)])


def everywhere(shard, axis):
    copies = jnp.broadcast_to(shard[None], (lax.axis_size(axis), *shard.shape))
    return lax.all_to_all(copies, axis, split_axis=0, concat_axis=0, tiled=True)


def summed_over(sums, groups):
    for group in groups:
        sums = everywhere(sums, group).sum(axis=0)
    return sums


def params():
    return pltpu.CompilerParams(vmem_limit_bytes=VMEM_LIMIT)


def longitude_kernel_body(high_ref, low_ref):
    rows, columns = high_ref.shape
    own = lax.broadcasted_iota(jnp.int32, (rows, columns), 0)
    other = lax.broadcasted_iota(jnp.int32, (rows, columns), 1)
    spacing = jnp.abs(own - other)
    spacing = jnp.minimum(spacing, NLON - spacing).astype(jnp.float32)
    value = jnp.exp(-0.5 * (spacing / LOCLON) ** 2)
    high = value.astype(jnp.bfloat16)
    high_ref[...] = high
    low_ref[...] = (value - high.astype(jnp.float32)).astype(jnp.bfloat16)


def longitude_kernel():
    part = jax.ShapeDtypeStruct((NLON, BLOCK), jnp.bfloat16)
    return pl.pallas_call(
        longitude_kernel_body,
        out_shape=(part, part),
        compiler_params=params(),
        cost_estimate=pl.CostEstimate(
            flops=20 * NLON * BLOCK, transcendentals=NLON * BLOCK, bytes_accessed=4 * NLON * BLOCK
        ),
        name="longitude_kernel",
    )()


def blend_body(ensemble_ref, low_ref, own_ref, high_ref, kernel_high_ref, kernel_low_ref, out_ref, ext_ref):
    members, variables, coarse_rows, columns = ensemble_ref.shape
    ext_rows = coarse_rows + 2 * LSTEPS
    bands = 1
    for axis in BAND:
        bands = bands * lax.axis_size(axis)
    band = lax.axis_index(BAND)
    for m in range(members):
        base = m * ext_rows
        ext_ref[base : base + LSTEPS] = low_ref[m]
        ext_ref[base + LSTEPS : base + LSTEPS + coarse_rows] = own_ref[m]
        ext_ref[base + LSTEPS + coarse_rows : base + ext_rows] = high_ref[m]
    q = ext_ref[...]
    total = members * ext_rows
    place = lax.rem(lax.broadcasted_iota(jnp.int32, (total, 1), 0), ext_rows)
    row = band * coarse_rows - LSTEPS + place
    rows = bands * coarse_rows
    north = jnp.where((row >= 0) & (row < rows - 1), LATITUDE_RATE, 0.0)
    south = jnp.where((row > 0) & (row <= rows - 1), LATITUDE_RATE, 0.0)
    for _ in range(LSTEPS):
        q = (
            q
            + north * (pltpu.roll(q, total - 1, 0) - q)
            + south * (pltpu.roll(q, 1, 0) - q)
        )
    ext_ref[...] = q
    x = jnp.concatenate(
        [
            ext_ref[m * ext_rows + LSTEPS : m * ext_rows + LSTEPS + coarse_rows]
            for m in range(members)
        ],
        axis=0,
    )
    turned = jnp.concatenate(
        [x] + [
            jnp.concatenate([x[:, BLOCK * j :], x[:, : BLOCK * j]], axis=1)
            for j in range(1, NLON // BLOCK)
        ],
        axis=0,
    )
    part = turned.astype(jnp.bfloat16)
    rest = (turned - part.astype(jnp.float32)).astype(jnp.bfloat16)
    kernel_high = kernel_high_ref[...]
    y = jnp.dot(part, kernel_high, preferred_element_type=jnp.float32)
    y = y + jnp.dot(rest, kernel_high, preferred_element_type=jnp.float32)
    y = y + jnp.dot(part, kernel_low_ref[...], preferred_element_type=jnp.float32)
    held = members * coarse_rows
    blended = jnp.concatenate(
        [y[held * j : held * (j + 1)] for j in range(NLON // BLOCK)], axis=1
    )
    for v in range(variables):
        term = ensemble_ref[0, v] * blended[:coarse_rows]
        for m in range(1, members):
            term = term + ensemble_ref[m, v] * blended[m * coarse_rows : (m + 1) * coarse_rows]
        out_ref[v] = term


def blend(ensemble, low, own, high, kernel_high, kernel_low):
    members, variables, coarse_rows, columns = ensemble.shape
    return pl.pallas_call(
        blend_body,
        out_shape=jax.ShapeDtypeStruct((variables, coarse_rows, columns), jnp.float32),
        scratch_shapes=[pltpu.VMEM((members * (coarse_rows + 2 * LSTEPS), columns), jnp.float32)],
        compiler_params=params(),
        cost_estimate=pl.CostEstimate(
            flops=6 * 16 * NLON * NLON, transcendentals=0, bytes_accessed=4 << 20
        ),
        name="blend",
    )(ensemble, low, own, high, kernel_high, kernel_low)


def diffuse_body(low_ref, own_ref, high_ref, out_ref, field_ref, east_ref, north_ref):
    twice, tile_rows, width = own_ref.shape
    variables = twice // 2
    height = 3 * tile_rows
    bands = 1
    for axis in BAND:
        bands = bands * lax.axis_size(axis)
    first = lax.axis_index(BAND) * tile_rows - tile_rows
    row = first + lax.broadcasted_iota(jnp.int32, (height, 1), 0)
    inside = (row >= 0) & (row + 1 <= bands * tile_rows - 1)
    for v in range(variables):
        field_ref[v] = jnp.concatenate([low_ref[v], own_ref[v], high_ref[v]], axis=0)
        w = variables + v
        rate = jnp.concatenate([low_ref[w], own_ref[w], high_ref[w]], axis=0)
        east_ref[v] = jnp.sqrt(rate * pltpu.roll(rate, width - 1, 1))
        north_ref[v] = jnp.where(inside, jnp.sqrt(rate * pltpu.roll(rate, height - 1, 0)), 0.0)

    def substep(_, carry):
        for v in range(variables):
            f = field_ref[v]
            east = east_ref[v] * (pltpu.roll(f, width - 1, 1) - f)
            north = north_ref[v] * (pltpu.roll(f, height - 1, 0) - f)
            change = east - pltpu.roll(east, 1, 1)
            change = change + north - pltpu.roll(north, 1, 0)
            field_ref[v] = f + change
        return carry

    lax.fori_loop(0, SUBSTEPS, substep, 0)
    for v in range(variables):
        out_ref[v] = field_ref[v, tile_rows : 2 * tile_rows, : out_ref.shape[2]]


def diffuse(low, own, high, columns):
    twice, tile_rows, width = own.shape
    variables = twice // 2
    held = pltpu.VMEM((variables, 3 * tile_rows, width), jnp.float32)
    return pl.pallas_call(
        diffuse_body,
        out_shape=jax.ShapeDtypeStruct((variables, tile_rows, columns), jnp.float32),
        scratch_shapes=[held, held, held],
        compiler_params=params(),
        cost_estimate=pl.CostEstimate(
            flops=16 * 12 * variables * 48 * width, transcendentals=0, bytes_accessed=2 << 20
        ),
        name="diffuse",
    )(low, own, high)


def chosen(rows, columns, ratio, by_row):
    own = lax.broadcasted_iota(jnp.int32, (rows, columns), 0)
    other = lax.broadcasted_iota(jnp.int32, (rows, columns), 1)
    same = (other // ratio == own) if by_row else (own // ratio == other)
    return same.astype(jnp.float32)


def shards(ensemble, gradient, previous, diffusivity):
    variables, tile_rows, columns = gradient.shape
    members, _, coarse_rows, _ = ensemble.shape
    coarse_cols = columns // REFINE
    owners = lax.axis_size(MEM)
    row_sums = gradient.reshape(variables * coarse_rows, REFINE, columns).sum(axis=1)
    restricted = jnp.dot(
        row_sums, chosen(columns, coarse_cols, REFINE, False), precision=lax.Precision.HIGHEST
    ) * (1.0 / (REFINE * REFINE))
    gathered = everywhere(restricted.reshape(variables, coarse_rows, coarse_cols), MEM)
    gathered = jnp.moveaxis(gathered, 0, 2).reshape(variables, coarse_rows, NLON)
    both = jnp.concatenate([gradient, diffusivity], axis=0)
    left = shifted(both[:, :, columns - SUBSTEPS :], MEM, 1)
    right = shifted(both[:, :, :SUBSTEPS], MEM, -1)
    spare = -(columns + 2 * SUBSTEPS) % 128
    gap = jnp.zeros((2 * variables, tile_rows, spare), jnp.float32)
    extended = jnp.concatenate([both, right, gap, left], axis=2)
    kernel_high, kernel_low = longitude_kernel()
    control = jnp.sum(ensemble * gathered[None], axis=1)
    control_low = shifted(control, BAND, 1)
    control_high = shifted(control, BAND, -1)
    rows_low = shifted(extended, BAND, 1)
    rows_high = shifted(extended, BAND, -1)
    member_terms = blend(ensemble, control_low, control, control_high, kernel_high, kernel_low)
    blocks = jnp.moveaxis(member_terms.reshape(variables, coarse_rows, owners, coarse_cols), 2, 0)
    arrived = lax.all_to_all(blocks, MEM, split_axis=0, concat_axis=0, tiled=True)
    smoothed = diffuse(rows_low, extended, rows_high, columns)
    inverse_count = 1.0 / (members * owners - 1)
    ensemble_part = arrived.sum(axis=0) * inverse_count
    spread = jnp.dot(
        ensemble_part.reshape(variables * coarse_rows, coarse_cols),
        chosen(coarse_cols, columns, REFINE, True),
        precision=lax.Precision.HIGHEST,
    )
    injected = jnp.broadcast_to(
        spread.reshape(variables, coarse_rows, 1, columns),
        (variables, coarse_rows, REFINE, columns),
    ).reshape(gradient.shape)
    direction = HYBRID_WEIGHT * smoothed + HYBRID_WEIGHT * injected
    along_sum, square_sum = summed_over(
        jnp.stack([jnp.sum(gradient * direction), jnp.sum(direction * direction)]), (MEM, BAND)
    )
    analysis = previous - along_sum / (along_sum + square_sum) * direction
    return (analysis, direction)


def solution(mesh):
    split = Mesh(
        mesh.devices.reshape(2, 8, 4, 8, 2), ("mem_0", "mem_1", "band_0", "band_1", "band_2")
    )
    return jax.shard_map(
        shards,
        mesh=split,
        in_specs=(
            P(MEM, None, BAND, None),
            P(None, BAND, MEM),
            P(None, BAND, MEM),
            P(None, BAND, MEM),
        ),
        out_specs=(P(None, BAND, MEM), P(None, BAND, MEM)),
        check_vma=False,
    )
```

```python
import functools

import jax
import jax.numpy as jnp
from jax import lax
from jax.experimental import pallas as pl
from jax.experimental.pallas import tpu as pltpu
from jax.sharding import Mesh
from jax.sharding import PartitionSpec as P

NLON = 1440
REFINE = 4
SUBSTEPS = 16
LSTEPS = 4
LOCLON = 48
BAND = ("band_0", "band_1", "band_2")
MEM = ("mem_0", "mem_1")
NEAR = ("mem_0", "mem_1", "band_2")
FAR = ("band_0", "band_1")

LATITUDE_RATE = 0.25
HYBRID_WEIGHT = 0.5
BLOCK = 240
VMEM_LIMIT = 24 << 20


def shifted(block, axis, step):
    count = lax.axis_size(axis)
    return lax.ppermute(block, axis, [(i, (i + step) % count) for i in range(count)])


def everywhere(shard, axis):
    copies = jnp.broadcast_to(shard[None], (lax.axis_size(axis), *shard.shape))
    return lax.all_to_all(copies, axis, split_axis=0, concat_axis=0, tiled=True)


def params():
    return pltpu.CompilerParams(vmem_limit_bytes=VMEM_LIMIT)


def longitude_kernel_body(high_ref, low_ref):
    rows, columns = high_ref.shape
    own = lax.broadcasted_iota(jnp.int32, (rows, columns), 0)
    other = lax.broadcasted_iota(jnp.int32, (rows, columns), 1)
    spacing = jnp.abs(own - other)
    spacing = jnp.minimum(spacing, NLON - spacing).astype(jnp.float32)
    value = jnp.exp(-0.5 * (spacing / LOCLON) ** 2)
    high = value.astype(jnp.bfloat16)
    high_ref[...] = high
    low_ref[...] = (value - high.astype(jnp.float32)).astype(jnp.bfloat16)


def longitude_kernel():
    part = jax.ShapeDtypeStruct((NLON, BLOCK), jnp.bfloat16)
    return pl.pallas_call(
        longitude_kernel_body,
        out_shape=(part, part),
        compiler_params=params(),
        cost_estimate=pl.CostEstimate(
            flops=20 * NLON * BLOCK, transcendentals=NLON * BLOCK, bytes_accessed=4 * NLON * BLOCK
        ),
        name="longitude_kernel",
    )()


def blend_body(ensemble_ref, low_ref, own_ref, high_ref, kernel_high_ref, kernel_low_ref, out_ref, ext_ref):
    members, variables, coarse_rows, columns = ensemble_ref.shape
    ext_rows = coarse_rows + 2 * LSTEPS
    bands = 1
    for axis in BAND:
        bands = bands * lax.axis_size(axis)
    band = lax.axis_index(BAND)
    for m in range(members):
        base = m * ext_rows
        ext_ref[base : base + LSTEPS] = low_ref[m]
        ext_ref[base + LSTEPS : base + LSTEPS + coarse_rows] = own_ref[m]
        ext_ref[base + LSTEPS + coarse_rows : base + ext_rows] = high_ref[m]
    q = ext_ref[...]
    total = members * ext_rows
    place = lax.rem(lax.broadcasted_iota(jnp.int32, (total, 1), 0), ext_rows)
    row = band * coarse_rows - LSTEPS + place
    rows = bands * coarse_rows
    north = jnp.where((row >= 0) & (row < rows - 1), LATITUDE_RATE, 0.0)
    south = jnp.where((row > 0) & (row <= rows - 1), LATITUDE_RATE, 0.0)
    for _ in range(LSTEPS):
        q = (
            q
            + north * (pltpu.roll(q, total - 1, 0) - q)
            + south * (pltpu.roll(q, 1, 0) - q)
        )
    ext_ref[...] = q
    x = jnp.concatenate(
        [
            ext_ref[m * ext_rows + LSTEPS : m * ext_rows + LSTEPS + coarse_rows]
            for m in range(members)
        ],
        axis=0,
    )
    turned = jnp.concatenate(
        [x] + [
            jnp.concatenate([x[:, BLOCK * j :], x[:, : BLOCK * j]], axis=1)
            for j in range(1, NLON // BLOCK)
        ],
        axis=0,
    )
    part = turned.astype(jnp.bfloat16)
    rest = (turned - part.astype(jnp.float32)).astype(jnp.bfloat16)
    kernel_high = kernel_high_ref[...]
    y = jnp.dot(part, kernel_high, preferred_element_type=jnp.float32)
    y = y + jnp.dot(rest, kernel_high, preferred_element_type=jnp.float32)
    y = y + jnp.dot(part, kernel_low_ref[...], preferred_element_type=jnp.float32)
    held = members * coarse_rows
    blended = jnp.concatenate(
        [y[held * j : held * (j + 1)] for j in range(NLON // BLOCK)], axis=1
    )
    for v in range(variables):
        term = ensemble_ref[0, v] * blended[:coarse_rows]
        for m in range(1, members):
            term = term + ensemble_ref[m, v] * blended[m * coarse_rows : (m + 1) * coarse_rows]
        out_ref[v] = term


def blend(ensemble, low, own, high, kernel_high, kernel_low):
    members, variables, coarse_rows, columns = ensemble.shape
    return pl.pallas_call(
        blend_body,
        out_shape=jax.ShapeDtypeStruct((variables, coarse_rows, columns), jnp.float32),
        scratch_shapes=[pltpu.VMEM((members * (coarse_rows + 2 * LSTEPS), columns), jnp.float32)],
        compiler_params=params(),
        cost_estimate=pl.CostEstimate(
            flops=6 * 16 * NLON * NLON, transcendentals=0, bytes_accessed=4 << 20
        ),
        name="blend",
    )(ensemble, low, own, high, kernel_high, kernel_low)


def diffuse_body(low_ref, own_ref, high_ref, out_ref, field_ref, east_ref, north_ref):
    twice, tile_rows, width = own_ref.shape
    variables = twice // 2
    height = 3 * tile_rows
    bands = 1
    for axis in BAND:
        bands = bands * lax.axis_size(axis)
    first = lax.axis_index(BAND) * tile_rows - tile_rows
    row = first + lax.broadcasted_iota(jnp.int32, (height, 1), 0)
    inside = (row >= 0) & (row + 1 <= bands * tile_rows - 1)
    for v in range(variables):
        field_ref[v] = jnp.concatenate([low_ref[v], own_ref[v], high_ref[v]], axis=0)
        w = variables + v
        rate = jnp.concatenate([low_ref[w], own_ref[w], high_ref[w]], axis=0)
        east_ref[v] = jnp.sqrt(rate * pltpu.roll(rate, width - 1, 1))
        north_ref[v] = jnp.where(inside, jnp.sqrt(rate * pltpu.roll(rate, height - 1, 0)), 0.0)

    half = SUBSTEPS // 2
    for low, high in ((0, height), (half, height - half)):

        def substep(_, carry, low=low, high=high):
            for v in range(variables):
                f = field_ref[v, low:high]
                east = east_ref[v, low:high] * (pltpu.roll(f, width - 1, 1) - f)
                north = north_ref[v, low:high] * (pltpu.roll(f, high - low - 1, 0) - f)
                change = east - pltpu.roll(east, 1, 1)
                change = change + north - pltpu.roll(north, 1, 0)
                field_ref[v, low:high] = f + change
            return carry

        lax.fori_loop(0, half, substep, 0)
    for v in range(variables):
        out_ref[v] = field_ref[v, tile_rows : 2 * tile_rows, : out_ref.shape[2]]


def diffuse(low, own, high, columns):
    twice, tile_rows, width = own.shape
    variables = twice // 2
    held = pltpu.VMEM((variables, 3 * tile_rows, width), jnp.float32)
    return pl.pallas_call(
        diffuse_body,
        out_shape=jax.ShapeDtypeStruct((variables, tile_rows, columns), jnp.float32),
        scratch_shapes=[held, held, held],
        compiler_params=params(),
        cost_estimate=pl.CostEstimate(
            flops=16 * 12 * variables * 48 * width, transcendentals=0, bytes_accessed=2 << 20
        ),
        name="diffuse",
    )(low, own, high)


def chosen(rows, columns):
    own = lax.broadcasted_iota(jnp.int32, (rows, columns), 0)
    other = lax.broadcasted_iota(jnp.int32, (rows, columns), 1)
    return (own // REFINE == other).astype(jnp.float32)


def combine_body(inverse_count, arrived_ref, smoothed_ref, gradient_ref, direction_ref, sums_ref):
    owners, variables, coarse_rows, coarse_cols = arrived_ref.shape
    columns = smoothed_ref.shape[2]
    part = arrived_ref[0]
    for k in range(1, owners):
        part = part + arrived_ref[k]
    part = jnp.concatenate([part[v] for v in range(variables)], axis=0) * inverse_count
    own = lax.broadcasted_iota(jnp.int32, (coarse_cols, columns), 0)
    other = lax.broadcasted_iota(jnp.int32, (coarse_cols, columns), 1)
    copies = jnp.where(lax.shift_right_logical(other, 2) == own, 1.0, 0.0)
    spread = jnp.dot(
        part, copies, precision=lax.Precision.HIGHEST, preferred_element_type=jnp.float32
    )
    along = jnp.zeros((coarse_rows * REFINE, columns), jnp.float32)
    square = along
    for v in range(variables):
        injected = jnp.concatenate(
            [
                jnp.broadcast_to(spread[i : i + 1], (REFINE, columns))
                for i in range(v * coarse_rows, (v + 1) * coarse_rows)
            ],
            axis=0,
        )
        direction = HYBRID_WEIGHT * smoothed_ref[v] + HYBRID_WEIGHT * injected
        direction_ref[v] = direction
        along = along + gradient_ref[v] * direction
        square = square + direction * direction
    along = jnp.sum(jnp.sum(along, axis=0, keepdims=True), axis=1, keepdims=True)
    square = jnp.sum(jnp.sum(square, axis=0, keepdims=True), axis=1, keepdims=True)
    lane = lax.broadcasted_iota(jnp.int32, sums_ref.shape, 1)
    sums_ref[...] = jnp.where(lane == 0, along, jnp.where(lane == 1, square, 0.0))


def combine(arrived, smoothed, gradient, inverse_count, peers):
    return pl.pallas_call(
        functools.partial(combine_body, inverse_count),
        out_shape=(
            jax.ShapeDtypeStruct(gradient.shape, jnp.float32),
            jax.ShapeDtypeStruct((peers, 128), jnp.float32),
        ),
        compiler_params=params(),
        cost_estimate=pl.CostEstimate(flops=8 << 20, transcendentals=0, bytes_accessed=1 << 20),
        name="combine",
    )(arrived, smoothed, gradient)


def step_body(sums_ref, direction_ref, previous_ref, analysis_ref, out_ref):
    sums = jnp.sum(sums_ref[...], axis=0, keepdims=True)
    along, square = sums[:, 0:1], sums[:, 1:2]
    length = along / (along + square)
    for v in range(direction_ref.shape[0]):
        direction = direction_ref[v]
        out_ref[v] = direction
        analysis_ref[v] = previous_ref[v] - length * direction


def step(sums, direction, previous):
    tile = jax.ShapeDtypeStruct(direction.shape, jnp.float32)
    return pl.pallas_call(
        step_body,
        out_shape=(tile, tile),
        compiler_params=params(),
        cost_estimate=pl.CostEstimate(flops=1 << 20, transcendentals=0, bytes_accessed=1 << 20),
        name="step",
    )(sums, direction, previous)


def shards(ensemble, gradient, previous, diffusivity):
    variables, tile_rows, columns = gradient.shape
    members, _, coarse_rows, _ = ensemble.shape
    coarse_cols = columns // REFINE
    owners = lax.axis_size(MEM)
    row_sums = gradient.reshape(variables * coarse_rows, REFINE, columns).sum(axis=1)
    restricted = jnp.dot(
        row_sums, chosen(columns, coarse_cols), precision=lax.Precision.HIGHEST
    ) * (1.0 / (REFINE * REFINE))
    gathered = everywhere(restricted.reshape(variables, coarse_rows, coarse_cols), MEM)
    gathered = jnp.moveaxis(gathered, 0, 2).reshape(variables, coarse_rows, NLON)
    both = jnp.concatenate([gradient, diffusivity], axis=0)
    left = shifted(both[:, :, columns - SUBSTEPS :], MEM, 1)
    right = shifted(both[:, :, :SUBSTEPS], MEM, -1)
    spare = -(columns + 2 * SUBSTEPS) % 128
    gap = jnp.zeros((2 * variables, tile_rows, spare), jnp.float32)
    extended = jnp.concatenate([both, right, gap, left], axis=2)
    kernel_high, kernel_low = longitude_kernel()
    control = jnp.sum(ensemble * gathered[None], axis=1)
    control_low = shifted(control, BAND, 1)
    control_high = shifted(control, BAND, -1)
    rows_low = shifted(extended, BAND, 1)
    rows_high = shifted(extended, BAND, -1)
    member_terms = blend(ensemble, control_low, control, control_high, kernel_high, kernel_low)
    blocks = jnp.moveaxis(member_terms.reshape(variables, coarse_rows, owners, coarse_cols), 2, 0)
    arrived = lax.all_to_all(blocks, MEM, split_axis=0, concat_axis=0, tiled=True)
    smoothed = diffuse(rows_low, extended, rows_high, columns)
    peers = lax.axis_size(NEAR)
    direction, sums = combine(
        arrived, smoothed, gradient, 1.0 / (members * owners - 1), peers
    )
    sums = lax.all_to_all(sums, NEAR, split_axis=0, concat_axis=0, tiled=True)
    sums = everywhere(sums.sum(axis=0, keepdims=True), FAR)
    return step(sums.reshape(-1, 128), direction, previous)


def solution(mesh):
    split = Mesh(
        mesh.devices.reshape(2, 8, 4, 8, 2), ("mem_0", "mem_1", "band_0", "band_1", "band_2")
    )
    return jax.shard_map(
        shards,
        mesh=split,
        in_specs=(
            P(MEM, None, BAND, None),
            P(None, BAND, MEM),
            P(None, BAND, MEM),
            P(None, BAND, MEM),
        ),
        out_specs=(P(None, BAND, MEM), P(None, BAND, MEM)),
        check_vma=False,
    )
```

```python
import functools

import jax
import jax.numpy as jnp
from jax import lax
from jax.experimental import pallas as pl
from jax.experimental.pallas import tpu as pltpu
from jax.sharding import Mesh
from jax.sharding import PartitionSpec as P

NLON = 1440
REFINE = 4
SUBSTEPS = 16
LSTEPS = 4
LOCLON = 48
BAND = ("band_0", "band_1", "band_2")
MEM = ("mem_0", "mem_1")
NEAR = ("mem_0", "mem_1", "band_2")
FAR = ("band_0", "band_1")

LATITUDE_RATE = 0.25
HYBRID_WEIGHT = 0.5
BLOCK = 240
VMEM_LIMIT = 24 << 20


def shifted(block, axis, step):
    count = lax.axis_size(axis)
    return lax.ppermute(block, axis, [(i, (i + step) % count) for i in range(count)])


def everywhere(shard, axis):
    copies = jnp.broadcast_to(shard[None], (lax.axis_size(axis), *shard.shape))
    return lax.all_to_all(copies, axis, split_axis=0, concat_axis=0, tiled=True)


def params():
    return pltpu.CompilerParams(vmem_limit_bytes=VMEM_LIMIT)


def longitude_kernel_body(high_ref, low_ref):
    rows, columns = high_ref.shape
    own = lax.broadcasted_iota(jnp.int32, (rows, columns), 0)
    other = lax.broadcasted_iota(jnp.int32, (rows, columns), 1)
    spacing = jnp.abs(own - other)
    spacing = jnp.minimum(spacing, NLON - spacing).astype(jnp.float32)
    value = jnp.exp(-0.5 * (spacing / LOCLON) ** 2)
    high = value.astype(jnp.bfloat16)
    high_ref[...] = high
    low_ref[...] = (value - high.astype(jnp.float32)).astype(jnp.bfloat16)


def longitude_kernel():
    part = jax.ShapeDtypeStruct((NLON, BLOCK), jnp.bfloat16)
    return pl.pallas_call(
        longitude_kernel_body,
        out_shape=(part, part),
        compiler_params=params(),
        cost_estimate=pl.CostEstimate(
            flops=20 * NLON * BLOCK, transcendentals=NLON * BLOCK, bytes_accessed=4 * NLON * BLOCK
        ),
        name="longitude_kernel",
    )()


def blend_body(ensemble_ref, low_ref, own_ref, high_ref, kernel_high_ref, kernel_low_ref, out_ref, ext_ref):
    members, variables, coarse_rows, columns = ensemble_ref.shape
    ext_rows = coarse_rows + 2 * LSTEPS
    bands = 1
    for axis in BAND:
        bands = bands * lax.axis_size(axis)
    band = lax.axis_index(BAND)
    held = members * coarse_rows
    width = own_ref.shape[1]
    pieces = range(0, columns, width)
    start = own_ref.shape[0] - held * len(pieces)
    for m in range(members):
        base = m * ext_rows
        for p, lane in enumerate(pieces):
            lanes = min(width, columns - lane)
            at = start + held * p + m * coarse_rows
            for k, ref in enumerate((low_ref, own_ref, high_ref)):
                ext_ref[base + coarse_rows * k : base + coarse_rows * (k + 1), lane : lane + lanes] = (
                    ref[at : at + coarse_rows, :lanes]
                )
    q = ext_ref[...]
    total = members * ext_rows
    place = lax.rem(lax.broadcasted_iota(jnp.int32, (total, 1), 0), ext_rows)
    row = band * coarse_rows - LSTEPS + place
    rows = bands * coarse_rows
    north = jnp.where((row >= 0) & (row < rows - 1), LATITUDE_RATE, 0.0)
    south = jnp.where((row > 0) & (row <= rows - 1), LATITUDE_RATE, 0.0)
    for _ in range(LSTEPS):
        q = (
            q
            + north * (pltpu.roll(q, total - 1, 0) - q)
            + south * (pltpu.roll(q, 1, 0) - q)
        )
    ext_ref[...] = q
    x = jnp.concatenate(
        [
            ext_ref[m * ext_rows + LSTEPS : m * ext_rows + LSTEPS + coarse_rows]
            for m in range(members)
        ],
        axis=0,
    )
    turned = jnp.concatenate(
        [x] + [
            jnp.concatenate([x[:, BLOCK * j :], x[:, : BLOCK * j]], axis=1)
            for j in range(1, NLON // BLOCK)
        ],
        axis=0,
    )
    part = turned.astype(jnp.bfloat16)
    rest = (turned - part.astype(jnp.float32)).astype(jnp.bfloat16)
    kernel_high = kernel_high_ref[...]
    y = jnp.dot(part, kernel_high, preferred_element_type=jnp.float32)
    y = y + jnp.dot(rest, kernel_high, preferred_element_type=jnp.float32)
    y = y + jnp.dot(part, kernel_low_ref[...], preferred_element_type=jnp.float32)
    blended = jnp.concatenate(
        [y[held * j : held * (j + 1)] for j in range(NLON // BLOCK)], axis=1
    )
    for v in range(variables):
        term = ensemble_ref[0, v] * blended[:coarse_rows]
        for m in range(1, members):
            term = term + ensemble_ref[m, v] * blended[m * coarse_rows : (m + 1) * coarse_rows]
        out_ref[v] = term


def blend(ensemble, low, own, high, kernel_high, kernel_low):
    members, variables, coarse_rows, columns = ensemble.shape
    return pl.pallas_call(
        blend_body,
        out_shape=jax.ShapeDtypeStruct((variables, coarse_rows, columns), jnp.float32),
        scratch_shapes=[pltpu.VMEM((members * (coarse_rows + 2 * LSTEPS), columns), jnp.float32)],
        compiler_params=params(),
        cost_estimate=pl.CostEstimate(
            flops=6 * 16 * NLON * NLON, transcendentals=0, bytes_accessed=4 << 20
        ),
        name="blend",
    )(ensemble, low, own, high, kernel_high, kernel_low)


def diffuse_body(low_ref, own_ref, high_ref, out_ref, stage_ref, field_ref, east_ref, north_ref):
    variables, tile_rows, _ = out_ref.shape
    width = own_ref.shape[1]
    height = 3 * tile_rows
    slots = height // 8
    bands = 1
    for axis in BAND:
        bands = bands * lax.axis_size(axis)
    first = lax.axis_index(BAND) * tile_rows - tile_rows
    sublane = lax.broadcasted_iota(jnp.int32, (8, 1), 0)

    def above(blocks):
        return blocks[1:] + [pltpu.roll(blocks[0], 7, 0)]

    def below(blocks):
        return [pltpu.roll(blocks[-1], 1, 0)] + blocks[:-1]

    def interleaved(w):
        for t in range(width // 128):
            lanes = slice(128 * t, 128 * (t + 1))
            for k, ref in enumerate((low_ref, own_ref, high_ref)):
                stage_ref[t, tile_rows * k : tile_rows * (k + 1)] = ref[
                    w * tile_rows : (w + 1) * tile_rows, lanes
                ]
        return [
            jnp.concatenate(
                [stage_ref[t, pl.ds(k, 8, stride=slots)] for t in range(width // 128)], axis=1
            )
            for k in range(slots)
        ]

    for v in range(variables):
        for k, f in enumerate(interleaved(v)):
            field_ref[v, k] = f
        rate = interleaved(variables + v)
        for k, (own, up) in enumerate(zip(rate, above(rate))):
            row = first + sublane * slots + k
            inside = (row >= 0) & (row + 1 <= bands * tile_rows - 1)
            east_ref[v, k] = jnp.sqrt(own * pltpu.roll(own, width - 1, 1))
            north_ref[v, k] = jnp.where(inside, jnp.sqrt(own * up), 0.0)

    def substep(_, carry):
        for v in range(variables):
            f = [field_ref[v, k] for k in range(slots)]
            up = above(f)
            north = [north_ref[v, k] * (up[k] - f[k]) for k in range(slots)]
            south = below(north)
            for k in range(slots):
                east = east_ref[v, k] * (pltpu.roll(f[k], width - 1, 1) - f[k])
                change = east - pltpu.roll(east, 1, 1)
                field_ref[v, k] = f[k] + (change + north[k] - south[k])
        return carry

    lax.fori_loop(0, SUBSTEPS, substep, 0)
    for v in range(variables):
        for t in range(width // 128):
            for k in range(slots):
                stage_ref[t, pl.ds(k, 8, stride=slots)] = field_ref[
                    v, k, :, 128 * t : 128 * (t + 1)
                ]
        tile = [stage_ref[t, tile_rows : 2 * tile_rows] for t in range(width // 128)]
        out_ref[v] = jnp.concatenate(tile, axis=1)[:, : out_ref.shape[2]]


def diffuse(low, own, high, shape):
    variables, tile_rows, columns = shape
    width = own.shape[1]
    held = pltpu.VMEM((variables, 3 * tile_rows // 8, 8, width), jnp.float32)
    return pl.pallas_call(
        diffuse_body,
        out_shape=jax.ShapeDtypeStruct((variables, tile_rows, columns), jnp.float32),
        scratch_shapes=[pltpu.VMEM((width // 128, 3 * tile_rows, 128), jnp.float32), held, held, held],
        compiler_params=params(),
        cost_estimate=pl.CostEstimate(
            flops=16 * 12 * variables * 48 * width, transcendentals=0, bytes_accessed=2 << 20
        ),
        name="diffuse",
    )(low, own, high)


def prepare_body(
    gradient_ref, diffusivity_ref, both_ref, left_ref, right_ref, restricted_ref, sems
):
    variables, tile_rows, columns = gradient_ref.shape
    edge = left_ref.shape[2]
    reads = [
        pltpu.make_async_copy(ref, both_ref.at[pl.ds(variables * k, variables)], sems.at[k])
        for k, ref in enumerate((gradient_ref, diffusivity_ref))
    ]
    for read in reads:
        read.start()
    for read in reads:
        read.wait()
    rows = []
    for w in range(2 * variables):
        block = both_ref[w]
        left_ref[w] = block[:, columns - edge :]
        right_ref[w] = block[:, :edge]
    for v in range(variables):
        for i in range(0, tile_rows, REFINE):
            rows.append(jnp.sum(both_ref[v, i : i + REFINE], axis=0, keepdims=True))
    coarse_cols = restricted_ref.shape[1]
    own = lax.broadcasted_iota(jnp.int32, (columns, coarse_cols), 0)
    other = lax.broadcasted_iota(jnp.int32, (columns, coarse_cols), 1)
    chosen = jnp.where(lax.shift_right_logical(own, 2) == other, 1.0, 0.0)
    total = jnp.dot(
        jnp.concatenate(rows, axis=0),
        chosen,
        precision=lax.Precision.HIGHEST,
        preferred_element_type=jnp.float32,
    )
    restricted_ref[...] = total * (1.0 / (REFINE * REFINE))


def prepare(gradient, diffusivity):
    variables, tile_rows, columns = gradient.shape
    edge = jax.ShapeDtypeStruct((2 * variables, tile_rows, SUBSTEPS), jnp.float32)
    return pl.pallas_call(
        prepare_body,
        out_shape=(
            jax.ShapeDtypeStruct((2 * variables, tile_rows, columns), jnp.float32),
            edge,
            edge,
            jax.ShapeDtypeStruct(
                (variables * tile_rows // REFINE, columns // REFINE), jnp.float32
            ),
        ),
        in_specs=[pl.BlockSpec(memory_space=pltpu.MemorySpace.HBM)] * 2,
        scratch_shapes=[pltpu.SemaphoreType.DMA((2,))],
        compiler_params=params(),
        cost_estimate=pl.CostEstimate(flops=4 << 20, transcendentals=0, bytes_accessed=1 << 20),
        name="prepare",
    )(gradient, diffusivity)


def combine_body(inverse_count, arrived_ref, smoothed_ref, gradient_ref, direction_ref, sums_ref):
    owners, variables, coarse_rows, coarse_cols = arrived_ref.shape
    columns = smoothed_ref.shape[2]
    part = arrived_ref[0]
    for k in range(1, owners):
        part = part + arrived_ref[k]
    part = jnp.concatenate([part[v] for v in range(variables)], axis=0) * inverse_count
    own = lax.broadcasted_iota(jnp.int32, (coarse_cols, columns), 0)
    other = lax.broadcasted_iota(jnp.int32, (coarse_cols, columns), 1)
    copies = jnp.where(lax.shift_right_logical(other, 2) == own, 1.0, 0.0)
    spread = jnp.dot(
        part, copies, precision=lax.Precision.HIGHEST, preferred_element_type=jnp.float32
    )
    along = jnp.zeros((coarse_rows * REFINE, columns), jnp.float32)
    square = along
    for v in range(variables):
        injected = jnp.concatenate(
            [
                jnp.broadcast_to(spread[i : i + 1], (REFINE, columns))
                for i in range(v * coarse_rows, (v + 1) * coarse_rows)
            ],
            axis=0,
        )
        direction = HYBRID_WEIGHT * smoothed_ref[v] + HYBRID_WEIGHT * injected
        direction_ref[v] = direction
        along = along + gradient_ref[v] * direction
        square = square + direction * direction
    along = jnp.sum(jnp.sum(along, axis=0, keepdims=True), axis=1, keepdims=True)
    square = jnp.sum(jnp.sum(square, axis=0, keepdims=True), axis=1, keepdims=True)
    lane = lax.broadcasted_iota(jnp.int32, sums_ref.shape, 1)
    sums_ref[...] = jnp.where(lane == 0, along, jnp.where(lane == 1, square, 0.0))


def combine(arrived, smoothed, gradient, inverse_count, peers):
    return pl.pallas_call(
        functools.partial(combine_body, inverse_count),
        out_shape=(
            jax.ShapeDtypeStruct(gradient.shape, jnp.float32),
            jax.ShapeDtypeStruct((peers, 128), jnp.float32),
        ),
        compiler_params=params(),
        cost_estimate=pl.CostEstimate(flops=8 << 20, transcendentals=0, bytes_accessed=1 << 20),
        name="combine",
    )(arrived, smoothed, gradient)


def step_body(sums_ref, direction_ref, previous_ref, analysis_ref, out_ref):
    sums = jnp.sum(sums_ref[...], axis=0, keepdims=True)
    along, square = sums[:, 0:1], sums[:, 1:2]
    length = along / (along + square)
    for v in range(direction_ref.shape[0]):
        direction = direction_ref[v]
        out_ref[v] = direction
        analysis_ref[v] = previous_ref[v] - length * direction


def step(sums, direction, previous):
    tile = jax.ShapeDtypeStruct(direction.shape, jnp.float32)
    return pl.pallas_call(
        step_body,
        out_shape=(tile, tile),
        compiler_params=params(),
        cost_estimate=pl.CostEstimate(flops=1 << 20, transcendentals=0, bytes_accessed=1 << 20),
        name="step",
    )(sums, direction, previous)


def shards(ensemble, gradient, previous, diffusivity):
    variables, tile_rows, columns = gradient.shape
    members, _, coarse_rows, _ = ensemble.shape
    coarse_cols = columns // REFINE
    owners = lax.axis_size(MEM)
    both, left, right, restricted = prepare(gradient, diffusivity)
    gathered = everywhere(restricted.reshape(variables, coarse_rows, coarse_cols), MEM)
    gathered = jnp.moveaxis(gathered, 0, 2).reshape(variables, coarse_rows, NLON)
    left = shifted(left, MEM, 1)
    right = shifted(right, MEM, -1)
    spare = -(columns + 2 * SUBSTEPS) % 128
    gap = jnp.zeros((2 * variables, tile_rows, spare), jnp.float32)
    extended = jnp.concatenate([both, right, gap, left], axis=2)
    width = extended.shape[2]
    kernel_high, kernel_low = longitude_kernel()
    control = jnp.sum(ensemble * gathered[None], axis=1).reshape(members * coarse_rows, NLON)
    control = jnp.pad(control, ((0, 0), (0, -NLON % width)))
    own = jnp.concatenate(
        [extended.reshape(-1, width)]
        + [control[:, k : k + width] for k in range(0, NLON, width)],
        axis=0,
    )
    low = shifted(own, BAND, 1)
    high = shifted(own, BAND, -1)
    member_terms = blend(ensemble, low, own, high, kernel_high, kernel_low)
    blocks = jnp.moveaxis(member_terms.reshape(variables, coarse_rows, owners, coarse_cols), 2, 0)
    arrived = lax.all_to_all(blocks, MEM, split_axis=0, concat_axis=0, tiled=True)
    smoothed = diffuse(low, own, high, gradient.shape)
    peers = lax.axis_size(NEAR)
    direction, sums = combine(
        arrived, smoothed, gradient, 1.0 / (members * owners - 1), peers
    )
    sums = lax.all_to_all(sums, NEAR, split_axis=0, concat_axis=0, tiled=True)
    sums = everywhere(sums.sum(axis=0, keepdims=True), FAR)
    return step(sums.reshape(-1, 128), direction, previous)


def solution(mesh):
    split = Mesh(
        mesh.devices.reshape(2, 8, 4, 8, 2), ("mem_0", "mem_1", "band_0", "band_1", "band_2")
    )
    return jax.shard_map(
        shards,
        mesh=split,
        in_specs=(
            P(MEM, None, BAND, None),
            P(None, BAND, MEM),
            P(None, BAND, MEM),
            P(None, BAND, MEM),
        ),
        out_specs=(P(None, BAND, MEM), P(None, BAND, MEM)),
        check_vma=False,
    )
```

```python
import functools

import jax
import jax.numpy as jnp
from jax import lax
from jax.experimental import pallas as pl
from jax.experimental.pallas import tpu as pltpu
from jax.sharding import Mesh
from jax.sharding import PartitionSpec as P


NLON = 1440
REFINE = 4
SUBSTEPS = 16
LSTEPS = 4
LOCLON = 48
BAND = ("band_0", "band_1", "band_2")
MEM = ("mem_0", "mem_1")
NEAR = ("mem_0", "mem_1", "band_2")
FAR = ("band_0", "band_1")

LATITUDE_RATE = 0.25
HYBRID_WEIGHT = 0.5
BLOCK = 240
VMEM_LIMIT = 24 << 20


def swapped(block, axis, odd):
    count = lax.axis_size(axis)
    pairs = [(i, ((i + odd) ^ 1) - odd) for i in range(count)]
    return lax.ppermute(block, axis, [(i, partner % count) for i, partner in pairs])


def is_even(axis):
    return lax.rem(lax.axis_index(axis), 2) == 0


def everywhere(shard, axis):
    copies = jnp.broadcast_to(shard[None], (lax.axis_size(axis), *shard.shape))
    return lax.all_to_all(copies, axis, split_axis=0, concat_axis=0, tiled=True)


def params():
    return pltpu.CompilerParams(vmem_limit_bytes=VMEM_LIMIT)


def longitude_kernel_body(high_ref, low_ref):
    rows, columns = high_ref.shape
    own = lax.broadcasted_iota(jnp.int32, (rows, columns), 0)
    other = lax.broadcasted_iota(jnp.int32, (rows, columns), 1)
    spacing = jnp.abs(own - other)
    spacing = jnp.minimum(spacing, NLON - spacing).astype(jnp.float32)
    value = jnp.exp(-0.5 * (spacing / LOCLON) ** 2)
    high = value.astype(jnp.bfloat16)
    high_ref[...] = high
    low_ref[...] = (value - high.astype(jnp.float32)).astype(jnp.bfloat16)


def longitude_kernel():
    part = jax.ShapeDtypeStruct((NLON, BLOCK), jnp.bfloat16)
    return pl.pallas_call(
        longitude_kernel_body,
        out_shape=(part, part),
        compiler_params=params(),
        cost_estimate=pl.CostEstimate(
            flops=20 * NLON * BLOCK, transcendentals=NLON * BLOCK, bytes_accessed=4 * NLON * BLOCK
        ),
        name="longitude_kernel",
    )()


def blend_body(ensemble_ref, near_ref, own_ref, far_ref, kernel_high_ref, kernel_low_ref, out_ref, ext_ref):
    members, variables, coarse_rows, _ = ensemble_ref.shape
    ext_rows = coarse_rows + 2 * LSTEPS
    bands = 1
    for axis in BAND:
        bands = bands * lax.axis_size(axis)
    band = lax.axis_index(BAND)
    even = lax.rem(band, 2) == 0
    for m in range(members):
        base = m * ext_rows
        near, far = near_ref[m], far_ref[m]
        ext_ref[base : base + LSTEPS] = jnp.where(even, far, near)
        ext_ref[base + LSTEPS : base + LSTEPS + coarse_rows] = own_ref[m]
        ext_ref[base + LSTEPS + coarse_rows : base + ext_rows] = jnp.where(even, near, far)
    q = ext_ref[...]
    total = members * ext_rows
    place = lax.rem(lax.broadcasted_iota(jnp.int32, (total, 1), 0), ext_rows)
    row = band * coarse_rows - LSTEPS + place
    rows = bands * coarse_rows
    north = jnp.where((row >= 0) & (row < rows - 1), LATITUDE_RATE, 0.0)
    south = jnp.where((row > 0) & (row <= rows - 1), LATITUDE_RATE, 0.0)
    for _ in range(LSTEPS):
        q = (
            q
            + north * (pltpu.roll(q, total - 1, 0) - q)
            + south * (pltpu.roll(q, 1, 0) - q)
        )
    ext_ref[...] = q
    x = jnp.concatenate(
        [
            ext_ref[m * ext_rows + LSTEPS : m * ext_rows + LSTEPS + coarse_rows]
            for m in range(members)
        ],
        axis=0,
    )
    turned = jnp.concatenate(
        [x] + [
            jnp.concatenate([x[:, BLOCK * j :], x[:, : BLOCK * j]], axis=1)
            for j in range(1, NLON // BLOCK)
        ],
        axis=0,
    )
    part = turned.astype(jnp.bfloat16)
    rest = (turned - part.astype(jnp.float32)).astype(jnp.bfloat16)
    kernel_high = kernel_high_ref[...]
    y = jnp.dot(part, kernel_high, preferred_element_type=jnp.float32)
    y = y + jnp.dot(rest, kernel_high, preferred_element_type=jnp.float32)
    y = y + jnp.dot(part, kernel_low_ref[...], preferred_element_type=jnp.float32)
    held = members * coarse_rows
    blended = jnp.concatenate(
        [y[held * j : held * (j + 1)] for j in range(NLON // BLOCK)], axis=1
    )
    for v in range(variables):
        term = ensemble_ref[0, v] * blended[:coarse_rows]
        for m in range(1, members):
            term = term + ensemble_ref[m, v] * blended[m * coarse_rows : (m + 1) * coarse_rows]
        out_ref[v] = term


def blend(ensemble, near, own, far, kernel_high, kernel_low):
    members, variables, coarse_rows, columns = ensemble.shape
    return pl.pallas_call(
        blend_body,
        out_shape=jax.ShapeDtypeStruct((variables, coarse_rows, columns), jnp.float32),
        scratch_shapes=[pltpu.VMEM((members * (coarse_rows + 2 * LSTEPS), columns), jnp.float32)],
        compiler_params=params(),
        cost_estimate=pl.CostEstimate(
            flops=6 * 16 * NLON * NLON, transcendentals=0, bytes_accessed=4 << 20
        ),
        name="blend",
    )(ensemble, near, own, far, kernel_high, kernel_low)


def diffuse_body(near_ref, own_ref, far_ref, out_ref, field_ref, east_ref, north_ref):
    twice, tile_rows, width = own_ref.shape
    variables = twice // 2
    height = 3 * tile_rows
    bands = 1
    for axis in BAND:
        bands = bands * lax.axis_size(axis)
    even = is_even(BAND)
    first = lax.axis_index(BAND) * tile_rows - tile_rows

    def stacked(w):
        near, far = near_ref[w], far_ref[w]
        below, above = jnp.where(even, far, near), jnp.where(even, near, far)
        return jnp.concatenate([below, own_ref[w], above], axis=0)

    row = first + lax.broadcasted_iota(jnp.int32, (height, 1), 0)
    inside = (row >= 0) & (row + 1 <= bands * tile_rows - 1)
    for v in range(variables):
        field_ref[v] = stacked(v)
        rate = stacked(variables + v)
        east_ref[v] = jnp.sqrt(rate * pltpu.roll(rate, width - 1, 1))
        north_ref[v] = jnp.where(inside, jnp.sqrt(rate * pltpu.roll(rate, height - 1, 0)), 0.0)

    half = SUBSTEPS // 2
    for low, high in ((0, height), (half, height - half)):

        def substep(_, carry, low=low, high=high):
            for v in range(variables):
                f = field_ref[v, low:high]
                east = east_ref[v, low:high] * (pltpu.roll(f, width - 1, 1) - f)
                north = north_ref[v, low:high] * (pltpu.roll(f, high - low - 1, 0) - f)
                change = east - pltpu.roll(east, 1, 1)
                change = change + north - pltpu.roll(north, 1, 0)
                field_ref[v, low:high] = f + change
            return carry

        lax.fori_loop(0, half, substep, 0)
    for v in range(variables):
        out_ref[v] = field_ref[v, tile_rows : 2 * tile_rows, : out_ref.shape[2]]


def diffuse(near, own, far, columns):
    twice, tile_rows, width = own.shape
    variables = twice // 2
    held = pltpu.VMEM((variables, 3 * tile_rows, width), jnp.float32)
    return pl.pallas_call(
        diffuse_body,
        out_shape=jax.ShapeDtypeStruct((variables, tile_rows, columns), jnp.float32),
        scratch_shapes=[held, held, held],
        compiler_params=params(),
        cost_estimate=pl.CostEstimate(
            flops=16 * 12 * variables * 48 * width, transcendentals=0, bytes_accessed=2 << 20
        ),
        name="diffuse",
    )(near, own, far)


def chosen(rows, columns):
    own = lax.broadcasted_iota(jnp.int32, (rows, columns), 0)
    other = lax.broadcasted_iota(jnp.int32, (rows, columns), 1)
    return (own // REFINE == other).astype(jnp.float32)


def combine_body(inverse_count, arrived_ref, smoothed_ref, gradient_ref, direction_ref, sums_ref):
    owners, variables, coarse_rows, coarse_cols = arrived_ref.shape
    columns = smoothed_ref.shape[2]
    part = arrived_ref[0]
    for k in range(1, owners):
        part = part + arrived_ref[k]
    part = jnp.concatenate([part[v] for v in range(variables)], axis=0) * inverse_count
    own = lax.broadcasted_iota(jnp.int32, (coarse_cols, columns), 0)
    other = lax.broadcasted_iota(jnp.int32, (coarse_cols, columns), 1)
    copies = jnp.where(lax.shift_right_logical(other, 2) == own, 1.0, 0.0)
    spread = jnp.dot(
        part, copies, precision=lax.Precision.HIGHEST, preferred_element_type=jnp.float32
    )
    along = jnp.zeros((coarse_rows * REFINE, columns), jnp.float32)
    square = along
    for v in range(variables):
        injected = jnp.concatenate(
            [
                jnp.broadcast_to(spread[i : i + 1], (REFINE, columns))
                for i in range(v * coarse_rows, (v + 1) * coarse_rows)
            ],
            axis=0,
        )
        direction = HYBRID_WEIGHT * smoothed_ref[v] + HYBRID_WEIGHT * injected
        direction_ref[v] = direction
        along = along + gradient_ref[v] * direction
        square = square + direction * direction
    along = jnp.sum(jnp.sum(along, axis=0, keepdims=True), axis=1, keepdims=True)
    square = jnp.sum(jnp.sum(square, axis=0, keepdims=True), axis=1, keepdims=True)
    lane = lax.broadcasted_iota(jnp.int32, sums_ref.shape, 1)
    sums_ref[...] = jnp.where(lane == 0, along, jnp.where(lane == 1, square, 0.0))


def combine(arrived, smoothed, gradient, inverse_count, peers):
    return pl.pallas_call(
        functools.partial(combine_body, inverse_count),
        out_shape=(
            jax.ShapeDtypeStruct(gradient.shape, jnp.float32),
            jax.ShapeDtypeStruct((peers, 128), jnp.float32),
        ),
        compiler_params=params(),
        cost_estimate=pl.CostEstimate(flops=8 << 20, transcendentals=0, bytes_accessed=1 << 20),
        name="combine",
    )(arrived, smoothed, gradient)


def step_body(sums_ref, direction_ref, previous_ref, analysis_ref, out_ref):
    sums = jnp.sum(sums_ref[...], axis=0, keepdims=True)
    along, square = sums[:, 0:1], sums[:, 1:2]
    length = along / (along + square)
    for v in range(direction_ref.shape[0]):
        direction = direction_ref[v]
        out_ref[v] = direction
        analysis_ref[v] = previous_ref[v] - length * direction


def step(sums, direction, previous):
    tile = jax.ShapeDtypeStruct(direction.shape, jnp.float32)
    return pl.pallas_call(
        step_body,
        out_shape=(tile, tile),
        compiler_params=params(),
        cost_estimate=pl.CostEstimate(flops=1 << 20, transcendentals=0, bytes_accessed=1 << 20),
        name="step",
    )(sums, direction, previous)


def shards(ensemble, gradient, previous, diffusivity):
    variables, tile_rows, columns = gradient.shape
    members, _, coarse_rows, _ = ensemble.shape
    coarse_cols = columns // REFINE
    owners = lax.axis_size(MEM)
    row_sums = gradient.reshape(variables * coarse_rows, REFINE, columns).sum(axis=1)
    restricted = jnp.dot(
        row_sums, chosen(columns, coarse_cols), precision=lax.Precision.HIGHEST
    ) * (1.0 / (REFINE * REFINE))
    payload = jnp.broadcast_to(
        restricted.reshape(1, variables, coarse_rows, coarse_cols),
        (owners, variables, coarse_rows, coarse_cols),
    )
    both = jnp.concatenate([gradient, diffusivity], axis=0)
    even = is_even(MEM)
    first, last = both[:, :, :SUBSTEPS], both[:, :, columns - SUBSTEPS :]
    up, down = jnp.where(even, last, first), jnp.where(even, first, last)
    gathered = lax.all_to_all(payload, MEM, split_axis=0, concat_axis=0, tiled=True)
    gathered = jnp.moveaxis(gathered, 0, 2).reshape(variables, coarse_rows, NLON)
    up, down = swapped(up, MEM, 0), swapped(down, MEM, 1)
    left, right = jnp.where(even, down, up), jnp.where(even, up, down)
    spare = -(columns + 2 * SUBSTEPS) % 128
    gap = jnp.zeros((2 * variables, tile_rows, spare), jnp.float32)
    extended = jnp.concatenate([both, right, gap, left], axis=2)
    kernel_high, kernel_low = longitude_kernel()
    control = jnp.sum(ensemble * gathered[None], axis=1)
    control_near = swapped(control, BAND, 0)
    control_far = swapped(control, BAND, 1)
    rows_near = swapped(extended, BAND, 0)
    rows_far = swapped(extended, BAND, 1)
    member_terms = blend(ensemble, control_near, control, control_far, kernel_high, kernel_low)
    blocks = jnp.moveaxis(member_terms.reshape(variables, coarse_rows, owners, coarse_cols), 2, 0)
    arrived = lax.all_to_all(blocks, MEM, split_axis=0, concat_axis=0, tiled=True)
    smoothed = diffuse(rows_near, extended, rows_far, columns)
    peers = lax.axis_size(NEAR)
    direction, sums = combine(
        arrived, smoothed, gradient, 1.0 / (members * owners - 1), peers
    )
    sums = lax.all_to_all(sums, NEAR, split_axis=0, concat_axis=0, tiled=True)
    sums = everywhere(sums.sum(axis=0, keepdims=True), FAR)
    return step(sums.reshape(-1, 128), direction, previous)


def solution(mesh):
    split = Mesh(
        mesh.devices.reshape(2, 8, 4, 8, 2), ("mem_0", "mem_1", "band_0", "band_1", "band_2")
    )
    return jax.shard_map(
        shards,
        mesh=split,
        in_specs=(
            P(MEM, None, BAND, None),
            P(None, BAND, MEM),
            P(None, BAND, MEM),
            P(None, BAND, MEM),
        ),
        out_specs=(P(None, BAND, MEM), P(None, BAND, MEM)),
        check_vma=False,
    )
```

```python
import functools

import jax
import jax.numpy as jnp
from jax import lax
from jax.experimental import pallas as pl
from jax.experimental.pallas import tpu as pltpu
from jax.sharding import Mesh
from jax.sharding import PartitionSpec as P


NLON = 1440
REFINE = 4
SUBSTEPS = 16
LSTEPS = 4
LOCLON = 48
BAND = ("band_0", "band_1", "band_2")
MEM = ("mem_0", "mem_1")
NEAR = ("mem_0", "mem_1", "band_2")
FAR = ("band_0", "band_1")

LATITUDE_RATE = 0.25
HYBRID_WEIGHT = 0.5
BLOCK = 240
VMEM_LIMIT = 24 << 20


def shifted(block, axis, step):
    count = lax.axis_size(axis)
    return lax.ppermute(block, axis, [(i, (i + step) % count) for i in range(count)])


def everywhere(shard, axis):
    copies = jnp.broadcast_to(shard[None], (lax.axis_size(axis), *shard.shape))
    return lax.all_to_all(copies, axis, split_axis=0, concat_axis=0, tiled=True)


def params():
    return pltpu.CompilerParams(vmem_limit_bytes=VMEM_LIMIT)


def longitude_kernel_body(high_ref, low_ref):
    rows, columns = high_ref.shape
    own = lax.broadcasted_iota(jnp.int32, (rows, columns), 0)
    other = lax.broadcasted_iota(jnp.int32, (rows, columns), 1)
    spacing = jnp.abs(own - other)
    spacing = jnp.minimum(spacing, NLON - spacing).astype(jnp.float32)
    value = jnp.exp(-0.5 * (spacing / LOCLON) ** 2)
    high = value.astype(jnp.bfloat16)
    high_ref[...] = high
    low_ref[...] = (value - high.astype(jnp.float32)).astype(jnp.bfloat16)


def longitude_kernel():
    part = jax.ShapeDtypeStruct((NLON, BLOCK), jnp.bfloat16)
    return pl.pallas_call(
        longitude_kernel_body,
        out_shape=(part, part),
        compiler_params=params(),
        cost_estimate=pl.CostEstimate(
            flops=20 * NLON * BLOCK, transcendentals=NLON * BLOCK, bytes_accessed=4 * NLON * BLOCK
        ),
        name="longitude_kernel",
    )()


def blend_body(ensemble_ref, low_ref, own_ref, high_ref, kernel_high_ref, kernel_low_ref, out_ref, ext_ref):
    members, variables, coarse_rows, _ = ensemble_ref.shape
    ext_rows = coarse_rows + 2 * LSTEPS
    bands = 1
    for axis in BAND:
        bands = bands * lax.axis_size(axis)
    band = lax.axis_index(BAND)
    for m in range(members):
        base = m * ext_rows
        ext_ref[base : base + LSTEPS] = low_ref[m]
        ext_ref[base + LSTEPS : base + LSTEPS + coarse_rows] = own_ref[m]
        ext_ref[base + LSTEPS + coarse_rows : base + ext_rows] = high_ref[m]
    q = ext_ref[...]
    total = members * ext_rows
    place = lax.rem(lax.broadcasted_iota(jnp.int32, (total, 1), 0), ext_rows)
    row = band * coarse_rows - LSTEPS + place
    rows = bands * coarse_rows
    north = jnp.where((row >= 0) & (row < rows - 1), LATITUDE_RATE, 0.0)
    south = jnp.where((row > 0) & (row <= rows - 1), LATITUDE_RATE, 0.0)
    for _ in range(LSTEPS):
        q = (
            q
            + north * (pltpu.roll(q, total - 1, 0) - q)
            + south * (pltpu.roll(q, 1, 0) - q)
        )
    ext_ref[...] = q
    x = jnp.concatenate(
        [
            ext_ref[m * ext_rows + LSTEPS : m * ext_rows + LSTEPS + coarse_rows]
            for m in range(members)
        ],
        axis=0,
    )
    turned = jnp.concatenate(
        [x] + [
            jnp.concatenate([x[:, BLOCK * j :], x[:, : BLOCK * j]], axis=1)
            for j in range(1, NLON // BLOCK)
        ],
        axis=0,
    )
    part = turned.astype(jnp.bfloat16)
    rest = (turned - part.astype(jnp.float32)).astype(jnp.bfloat16)
    kernel_high = kernel_high_ref[...]
    y = jnp.dot(part, kernel_high, preferred_element_type=jnp.float32)
    y = y + jnp.dot(rest, kernel_high, preferred_element_type=jnp.float32)
    y = y + jnp.dot(part, kernel_low_ref[...], preferred_element_type=jnp.float32)
    held = members * coarse_rows
    blended = jnp.concatenate(
        [y[held * j : held * (j + 1)] for j in range(NLON // BLOCK)], axis=1
    )
    for v in range(variables):
        term = ensemble_ref[0, v] * blended[:coarse_rows]
        for m in range(1, members):
            term = term + ensemble_ref[m, v] * blended[m * coarse_rows : (m + 1) * coarse_rows]
        out_ref[v] = term


def blend(ensemble, low, own, high, kernel_high, kernel_low):
    members, variables, coarse_rows, columns = ensemble.shape
    return pl.pallas_call(
        blend_body,
        out_shape=jax.ShapeDtypeStruct((variables, coarse_rows, columns), jnp.float32),
        scratch_shapes=[pltpu.VMEM((members * (coarse_rows + 2 * LSTEPS), columns), jnp.float32)],
        compiler_params=params(),
        cost_estimate=pl.CostEstimate(
            flops=6 * 16 * NLON * NLON, transcendentals=0, bytes_accessed=4 << 20
        ),
        name="blend",
    )(ensemble, low, own, high, kernel_high, kernel_low)


def diffuse_body(low_ref, own_ref, high_ref, out_ref, field_ref, east_ref, north_ref):
    twice, tile_rows, width = own_ref.shape
    variables = twice // 2
    height = 3 * tile_rows
    bands = 1
    for axis in BAND:
        bands = bands * lax.axis_size(axis)
    first = lax.axis_index(BAND) * tile_rows - tile_rows
    row = first + lax.broadcasted_iota(jnp.int32, (height, 1), 0)
    inside = (row >= 0) & (row + 1 <= bands * tile_rows - 1)
    for v in range(variables):
        field_ref[v] = jnp.concatenate([low_ref[v], own_ref[v], high_ref[v]], axis=0)
        w = variables + v
        rate = jnp.concatenate([low_ref[w], own_ref[w], high_ref[w]], axis=0)
        east_ref[v] = jnp.sqrt(rate * pltpu.roll(rate, width - 1, 1))
        north_ref[v] = jnp.where(inside, jnp.sqrt(rate * pltpu.roll(rate, height - 1, 0)), 0.0)

    half = SUBSTEPS // 2
    for low, high in ((0, height), (half, height - half)):

        def substep(_, carry, low=low, high=high):
            for v in range(variables):
                f = field_ref[v, low:high]
                east = east_ref[v, low:high] * (pltpu.roll(f, width - 1, 1) - f)
                north = north_ref[v, low:high] * (pltpu.roll(f, high - low - 1, 0) - f)
                change = east - pltpu.roll(east, 1, 1)
                change = change + north - pltpu.roll(north, 1, 0)
                field_ref[v, low:high] = f + change
            return carry

        lax.fori_loop(0, half, substep, 0)
    for v in range(variables):
        out_ref[v] = field_ref[v, tile_rows : 2 * tile_rows, : out_ref.shape[2]]


def diffuse(low, own, high, columns):
    twice, tile_rows, width = own.shape
    variables = twice // 2
    held = pltpu.VMEM((variables, 3 * tile_rows, width), jnp.float32)
    return pl.pallas_call(
        diffuse_body,
        out_shape=jax.ShapeDtypeStruct((variables, tile_rows, columns), jnp.float32),
        scratch_shapes=[held, held, held],
        compiler_params=params(),
        cost_estimate=pl.CostEstimate(
            flops=16 * 12 * variables * 48 * width, transcendentals=0, bytes_accessed=2 << 20
        ),
        name="diffuse",
    )(low, own, high)


def prepare_body(
    gradient_ref, diffusivity_ref, both_ref, left_ref, right_ref, restricted_ref, sems
):
    variables, tile_rows, columns = gradient_ref.shape
    edge = left_ref.shape[2]
    reads = [
        pltpu.make_async_copy(ref, both_ref.at[pl.ds(variables * k, variables)], sems.at[k])
        for k, ref in enumerate((gradient_ref, diffusivity_ref))
    ]
    for read in reads:
        read.start()
    for read in reads:
        read.wait()
    rows = []
    for w in range(2 * variables):
        block = both_ref[w]
        left_ref[w] = block[:, columns - edge :]
        right_ref[w] = block[:, :edge]
    for v in range(variables):
        for i in range(0, tile_rows, REFINE):
            rows.append(jnp.sum(both_ref[v, i : i + REFINE], axis=0, keepdims=True))
    coarse_cols = restricted_ref.shape[1]
    own = lax.broadcasted_iota(jnp.int32, (columns, coarse_cols), 0)
    other = lax.broadcasted_iota(jnp.int32, (columns, coarse_cols), 1)
    chosen = jnp.where(lax.shift_right_logical(own, 2) == other, 1.0, 0.0)
    total = jnp.dot(
        jnp.concatenate(rows, axis=0),
        chosen,
        precision=lax.Precision.HIGHEST,
        preferred_element_type=jnp.float32,
    )
    restricted_ref[...] = total * (1.0 / (REFINE * REFINE))


def prepare(gradient, diffusivity):
    variables, tile_rows, columns = gradient.shape
    edge = jax.ShapeDtypeStruct((2 * variables, tile_rows, SUBSTEPS), jnp.float32)
    return pl.pallas_call(
        prepare_body,
        out_shape=(
            jax.ShapeDtypeStruct((2 * variables, tile_rows, columns), jnp.float32),
            edge,
            edge,
            jax.ShapeDtypeStruct(
                (variables * tile_rows // REFINE, columns // REFINE), jnp.float32
            ),
        ),
        in_specs=[pl.BlockSpec(memory_space=pltpu.MemorySpace.HBM)] * 2,
        scratch_shapes=[pltpu.SemaphoreType.DMA((2,))],
        compiler_params=params(),
        cost_estimate=pl.CostEstimate(flops=4 << 20, transcendentals=0, bytes_accessed=1 << 20),
        name="prepare",
    )(*[pltpu.with_memory_space_constraint(x, pltpu.HBM) for x in (gradient, diffusivity)])


def combine_body(inverse_count, arrived_ref, smoothed_ref, gradient_ref, direction_ref, sums_ref):
    owners, variables, coarse_rows, coarse_cols = arrived_ref.shape
    columns = smoothed_ref.shape[2]
    part = arrived_ref[0]
    for k in range(1, owners):
        part = part + arrived_ref[k]
    part = jnp.concatenate([part[v] for v in range(variables)], axis=0) * inverse_count
    own = lax.broadcasted_iota(jnp.int32, (coarse_cols, columns), 0)
    other = lax.broadcasted_iota(jnp.int32, (coarse_cols, columns), 1)
    copies = jnp.where(lax.shift_right_logical(other, 2) == own, 1.0, 0.0)
    spread = jnp.dot(
        part, copies, precision=lax.Precision.HIGHEST, preferred_element_type=jnp.float32
    )
    along = jnp.zeros((coarse_rows * REFINE, columns), jnp.float32)
    square = along
    for v in range(variables):
        injected = jnp.concatenate(
            [
                jnp.broadcast_to(spread[i : i + 1], (REFINE, columns))
                for i in range(v * coarse_rows, (v + 1) * coarse_rows)
            ],
            axis=0,
        )
        direction = HYBRID_WEIGHT * smoothed_ref[v] + HYBRID_WEIGHT * injected
        direction_ref[v] = direction
        along = along + gradient_ref[v] * direction
        square = square + direction * direction
    along = jnp.sum(jnp.sum(along, axis=0, keepdims=True), axis=1, keepdims=True)
    square = jnp.sum(jnp.sum(square, axis=0, keepdims=True), axis=1, keepdims=True)
    lane = lax.broadcasted_iota(jnp.int32, sums_ref.shape, 1)
    sums_ref[...] = jnp.where(lane == 0, along, jnp.where(lane == 1, square, 0.0))


def combine(arrived, smoothed, gradient, inverse_count, peers):
    return pl.pallas_call(
        functools.partial(combine_body, inverse_count),
        out_shape=(
            jax.ShapeDtypeStruct(gradient.shape, jnp.float32),
            jax.ShapeDtypeStruct((peers, 128), jnp.float32),
        ),
        compiler_params=params(),
        cost_estimate=pl.CostEstimate(flops=8 << 20, transcendentals=0, bytes_accessed=1 << 20),
        name="combine",
    )(arrived, smoothed, gradient)


def step_body(sums_ref, direction_ref, previous_ref, analysis_ref, out_ref):
    sums = jnp.sum(sums_ref[...], axis=0, keepdims=True)
    along, square = sums[:, 0:1], sums[:, 1:2]
    length = along / (along + square)
    for v in range(direction_ref.shape[0]):
        direction = direction_ref[v]
        out_ref[v] = direction
        analysis_ref[v] = previous_ref[v] - length * direction


def step(sums, direction, previous):
    tile = jax.ShapeDtypeStruct(direction.shape, jnp.float32)
    return pl.pallas_call(
        step_body,
        out_shape=(tile, tile),
        compiler_params=params(),
        cost_estimate=pl.CostEstimate(flops=1 << 20, transcendentals=0, bytes_accessed=1 << 20),
        name="step",
    )(sums, direction, previous)


def shards(ensemble, gradient, previous, diffusivity):
    variables, tile_rows, columns = gradient.shape
    members, _, coarse_rows, _ = ensemble.shape
    coarse_cols = columns // REFINE
    owners = lax.axis_size(MEM)
    both, left, right, restricted = prepare(gradient, diffusivity)
    gathered = everywhere(restricted.reshape(variables, coarse_rows, coarse_cols), MEM)
    gathered = jnp.moveaxis(gathered, 0, 2).reshape(variables, coarse_rows, NLON)
    left = shifted(left, MEM, 1)
    right = shifted(right, MEM, -1)
    spare = -(columns + 2 * SUBSTEPS) % 128
    gap = jnp.zeros((2 * variables, tile_rows, spare), jnp.float32)
    extended = jnp.concatenate([both, right, gap, left], axis=2)
    kernel_high, kernel_low = longitude_kernel()
    control = jnp.sum(ensemble * gathered[None], axis=1)
    control_low = shifted(control, BAND, 1)
    control_high = shifted(control, BAND, -1)
    rows_low = shifted(extended, BAND, 1)
    rows_high = shifted(extended, BAND, -1)
    member_terms = blend(ensemble, control_low, control, control_high, kernel_high, kernel_low)
    blocks = jnp.moveaxis(member_terms.reshape(variables, coarse_rows, owners, coarse_cols), 2, 0)
    arrived = lax.all_to_all(blocks, MEM, split_axis=0, concat_axis=0, tiled=True)
    smoothed = diffuse(rows_low, extended, rows_high, columns)
    peers = lax.axis_size(NEAR)
    direction, sums = combine(
        arrived, smoothed, gradient, 1.0 / (members * owners - 1), peers
    )
    sums = lax.all_to_all(sums, NEAR, split_axis=0, concat_axis=0, tiled=True)
    sums = everywhere(sums.sum(axis=0, keepdims=True), FAR)
    return step(sums.reshape(-1, 128), direction, previous)


def solution(mesh):
    split = Mesh(
        mesh.devices.reshape(2, 8, 4, 8, 2), ("mem_0", "mem_1", "band_0", "band_1", "band_2")
    )
    return jax.shard_map(
        shards,
        mesh=split,
        in_specs=(
            P(MEM, None, BAND, None),
            P(None, BAND, MEM),
            P(None, BAND, MEM),
            P(None, BAND, MEM),
        ),
        out_specs=(P(None, BAND, MEM), P(None, BAND, MEM)),
        check_vma=False,
    )
```
